32 devices in a mesh: dp: 4 (over y, z), vp: 8 (over x, core).
Axes of the slice: x: 4, y: 2, z: 2, core: 2. Of those that a mesh axis runs over, the one named last changes fastest.
The devices are a block of a 4x4x8 slice.
Arguments:
- hidden: bfloat16 [8192, 3584], P(('dp', 'vp')), parts along dimension 0
- target: int32 [8192], P('dp'), parts along dimension 0
- norm_gain: bfloat16 [3584], replicated
- head_weight: bfloat16 [3584, 152064], P(None, 'vp')
Outputs:
- output 1: float32 [8192], P('dp'), parts along dimension 0
- output 2: float32 [8192], P('dp'), parts along dimension 0
- output 3: float32 [4], P('dp'), parts along dimension 0
There are 4 independent parts. The reference program is written for one: setup_inputs(seed, part) draws one part's arguments, and reference() takes and returns one part's arrays. A program takes and returns all parts, laid end to end along the dimension named above; an argument that names none is the same for every part.
All inputs are finite; a program needn't handle non-finite values.
Results may differ from the reference program's by a relative error of at most 0.001.
Values are sent between devices in bfloat16 or wider.
A program may use at most 768 MiB of HBM per device.

```python
import math
import jax
import jax.numpy as jnp
from jax import lax

D = 3584
VOCAB = 152064
TOK_DEV = 256
GROUP = 8
HEAD_BLOCK = 128
NORM_EPS = 1e-6
TOKENS = TOK_DEV * GROUP
ROW_BLOCK = math.gcd(TOKENS, 64)


def setup_inputs(seed: int = 0, part: int = 0) -> dict:
    key = jax.random.key(seed)
    part_key = jax.random.fold_in(key, part)
    hidden_key, target_key = jax.random.split(part_key)
    gain_key, head_key = jax.random.split(jax.random.fold_in(key, 1000003))
    hidden = jax.random.normal(hidden_key, (TOKENS, D), jnp.float32).astype(jnp.bfloat16)
    target = jax.random.randint(target_key, (TOKENS,), 0, VOCAB, jnp.int32)
    target = target.at[0].set(0).at[TOKENS - 1].set(VOCAB - 1)
    norm_gain = (1.0 + 0.5 * jax.random.normal(gain_key, (D,), jnp.float32)).astype(jnp.bfloat16)
    head_scale = 1.5 / math.sqrt(D)

    def draw_rows(row_key):
        return (jax.random.normal(row_key, (HEAD_BLOCK, VOCAB), jnp.float32) * head_scale).astype(jnp.bfloat16)

    head_weight = lax.map(draw_rows, jax.random.split(head_key, D // HEAD_BLOCK)).reshape(D, VOCAB)
    return {"hidden": hidden, "target": target, "norm_gain": norm_gain, "head_weight": head_weight}


def reference(hidden, target, norm_gain, head_weight):
    hidden_f32 = hidden.astype(jnp.float32)
    inv_rms = lax.rsqrt(jnp.mean(hidden_f32 * hidden_f32, axis=-1, keepdims=True) + NORM_EPS)
    normed = (hidden_f32 * inv_rms * norm_gain.astype(jnp.float32)).astype(jnp.bfloat16)
    vocab_ids = jnp.arange(VOCAB, dtype=jnp.int32)

    def score_block(block_args):
        block_rows, block_target = block_args
        logits = jnp.dot(block_rows, head_weight, preferred_element_type=jnp.float32)
        row_max = jnp.max(logits, axis=-1, keepdims=True)
        shifted = logits - row_max
        exp_vals = jnp.exp(shifted)
        exp_total = jnp.sum(exp_vals, axis=-1)
        moment = jnp.sum(exp_vals * shifted, axis=-1)
        target_shift = jnp.sum(jnp.where(vocab_ids[None, :] == block_target[:, None], shifted, 0.0), axis=-1)
        log_total = jnp.log(exp_total)
        return target_shift - log_total, log_total - moment / exp_total

    num_blocks = TOKENS // ROW_BLOCK
    log_prob, entropy = lax.map(score_block, (normed.reshape(num_blocks, ROW_BLOCK, D), target.reshape(num_blocks, ROW_BLOCK)))
    log_prob = log_prob.reshape(TOKENS)
    entropy = entropy.reshape(TOKENS)
    return log_prob, entropy, jnp.mean(log_prob).reshape(1)
```

```python
import functools

import jax
import jax.numpy as jnp
from jax import lax
from jax.experimental import pallas as pl
from jax.experimental.pallas import tpu as pltpu
from jax.sharding import PartitionSpec as P

NORM_EPS = 1e-6
LANES = 128
SUBLANES = 8
SUB = 528
PER_TILE = 2
NBUF = 4
LOWEST = float(jnp.finfo(jnp.float32).min)
MESH = pl.DeviceIdType.MESH


def kernel(
    n_dev, hidden_ref, target_ref, gain_ref, head_ref,
    lp_ref, ent_ref, mean_ref,
    rows_ref, w_ref, m_ref, z_ref, s_ref, t_ref, id_ref, buf_a, buf_b, pack_ref, all_ref,
    w_sem, send_sem, recv_sem, st_send, st_recv,
):
    own = hidden_ref.shape[0]
    half = own // 2
    chip_rows = 2 * own
    n_chip = n_dev // 2
    vocab = head_ref.shape[0]
    tile = PER_TILE * SUB
    tiles = vocab // tile
    pairs = tiles // 2
    groups = chip_rows // LANES
    me = lax.axis_index("vp")
    core = lax.rem(me, 2)
    chip = me // 2
    partner = me + 1 - 2 * core
    right = lax.rem(me + 2, n_dev)
    left = lax.rem(me + n_dev - 2, n_dev)

    def w_copy(g):
        row = lax.rem(g, tiles) * tile
        slot = lax.rem(g, NBUF)
        return pltpu.make_async_copy(
            head_ref.at[pl.ds(pl.multiple_of(row, tile), tile), :], w_ref.at[slot], w_sem.at[slot]
        )

    w_copy(0).start()
    w_copy(1).start()

    barrier = pltpu.get_barrier_semaphore()
    for j in range(1, n_dev):
        pl.semaphore_signal(barrier, inc=1, device_id={"vp": lax.rem(me + j, n_dev)}, device_id_type=MESH)

    gain = gain_ref[...].astype(jnp.float32).reshape(1, gain_ref.shape[-1])
    step = 32

    def norm(i, carry):
        x = hidden_ref[pl.ds(pl.multiple_of(i * step, step), step), :].astype(jnp.float32)
        inv = lax.rsqrt(jnp.mean(x * x, axis=-1, keepdims=True) + NORM_EPS)
        rows_ref[0, pl.ds(pl.multiple_of(core * own + i * step, step), step), :] = (x * inv * gain).astype(jnp.bfloat16)
        return carry

    lax.fori_loop(0, own // step, norm, 0)
    pl.semaphore_wait(barrier, n_dev - 1)

    def remote(src, dst, idx, device):
        return pltpu.make_async_remote_copy(
            src_ref=src, dst_ref=dst, send_sem=send_sem.at[idx], recv_sem=recv_sem.at[idx],
            device_id={"vp": device}, device_id_type=MESH,
        )

    mine = pl.multiple_of(core * own, own)

    def piece(slot, part):
        return rows_ref.at[slot, pl.ds(pl.multiple_of(core * own + part * half, half), half), :]

    whole = rows_ref.at[0, pl.ds(mine, own), :]
    to_partner = remote(whole, whole, 0, partner)
    right_a = remote(piece(0, 0), piece(3, 0), 1, right)
    left_b = remote(piece(0, 1), piece(1, 1), 2, left)
    right_b = remote(piece(0, 1), piece(3, 1), 3, right)
    left_a = remote(piece(0, 0), piece(1, 0), 4, left)
    fwd_a = remote(piece(3, 0), piece(2, 0), 5, right)
    fwd_b = remote(piece(1, 1), piece(2, 1), 6, left)
    relay = [
        remote(piece(slot, part), piece(slot, part), 7 + i, partner)
        for i, (slot, part) in enumerate([(3, 0), (1, 1), (3, 1), (1, 0), (2, 0), (2, 1)])
    ]
    to_partner.start()
    right_a.start()
    left_b.start()
    right_b.start()
    left_a.start()

    sublane = lax.broadcasted_iota(jnp.int32, (SUBLANES, LANES), 0)
    for k in range(n_chip):
        src = lax.rem(chip + k, n_chip)
        for g in range(groups):
            ids = target_ref[src, pl.ds(g, 1), :] - me * vocab
            ids = jnp.where((ids >= 0) & (ids < vocab), ids, -(2**29))
            id_ref[k, :, pl.ds(g * LANES, LANES)] = ids - sublane
    m_ref[...] = jnp.full(m_ref.shape, LOWEST, jnp.float32)
    z_ref[...] = jnp.zeros(z_ref.shape, jnp.float32)
    s_ref[...] = jnp.zeros(s_ref.shape, jnp.float32)
    t_ref[...] = jnp.zeros(t_ref.shape, jnp.float32)
    buf_b[...] = jnp.full(buf_b.shape, LOWEST, jnp.float32)

    def epilogue(buf, k, base):
        n = SUB // SUBLANES
        for g in range(groups):
            ls = pl.ds(g * LANES, LANES)

            def logits(r):
                return buf[pl.ds(r * SUBLANES, SUBLANES), ls]

            tops = [functools.reduce(jnp.maximum, [logits(r) for r in range(q, n, 4)]) for q in range(4)]
            m_old = m_ref[k, :, ls]
            m_new = functools.reduce(jnp.maximum, tops, m_old)
            d = jnp.maximum(m_old - m_new, -200.0)
            a = jnp.exp(d)
            zv = z_ref[k, :, ls]
            sv = a * (s_ref[k, :, ls] + d * zv)
            zv = a * zv
            tv = t_ref[k, :, ls]
            ids = id_ref[k, :, ls] - base
            for r in range(n):
                v = logits(r)
                d = v - m_new
                p = jnp.exp(d)
                zv = zv + p
                sv = sv + p * d
                tv = jnp.where(ids == r * SUBLANES, v, tv)
            m_ref[k, :, ls] = m_new
            z_ref[k, :, ls] = zv
            s_ref[k, :, ls] = sv
            t_ref[k, :, ls] = tv

    def block(k, slot, c, buf):
        buf[...] = lax.dot_general(
            w_ref[slot, pl.ds(c, SUB), :], rows_ref[k], (((1,), (1,)), ((), ())), preferred_element_type=jnp.float32
        )

    bufs = (buf_a, buf_b)

    to_partner.wait_recv()

    def first(i, carry):
        w_copy(2 * i + 2).start()
        w_copy(2 * i + 3).start()

        @pl.when(i == pairs * 3 // 9)
        def _():
            right_a.wait_recv()
            left_b.wait_recv()
            fwd_a.start()
            fwd_b.start()
            relay[0].start()
            relay[1].start()

        @pl.when(i == pairs * 6 // 9)
        def _():
            right_b.wait_recv()
            left_a.wait_recv()
            relay[2].start()
            relay[3].start()

        @pl.when(i == pairs - 1)
        def _():
            fwd_a.wait_recv()
            fwd_b.wait_recv()
            relay[4].start()
            relay[5].start()

        w_copy(2 * i).wait()
        w_copy(2 * i + 1).wait()
        for b in range(2 * PER_TILE):
            block(0, lax.rem(2 * i + b // PER_TILE, NBUF), (b % PER_TILE) * SUB, bufs[b % 2])
            epilogue(bufs[(b + 1) % 2], 0, i * 2 * tile + (b - 1) * SUB)
        return carry

    lax.fori_loop(0, pairs, first, 0)
    epilogue(buf_b, 0, vocab - SUB)
    buf_b[...] = jnp.full(buf_b.shape, LOWEST, jnp.float32)
    for r in relay:
        r.wait_recv()

    order = [(k, c) for c in range(0, tile, SUB) for k in range(1, n_chip)]

    def second(j, carry):
        g = tiles + j

        @pl.when(j < tiles - 2)
        def _():
            w_copy(g + 2).start()

        w_copy(g).wait()
        for b, (k, c) in enumerate(order):
            block(k, lax.rem(g, NBUF), c, bufs[b % 2])
            pk, pc = order[b - 1]
            epilogue(bufs[(b + 1) % 2], pk, j * tile + pc - (tile if b == 0 else 0))
        return carry

    lax.fori_loop(0, tiles, second, 0)
    epilogue(buf_b, n_chip - 1, vocab - SUB)

    for k in range(n_chip):
        dst = lax.rem(chip + k, n_chip)
        for g in range(groups):
            ls = pl.ds(g * LANES, LANES)
            m = m_ref[k, :, ls]
            top = jnp.max(m, axis=0, keepdims=True)
            d = jnp.maximum(m - top, -200.0)
            a = jnp.exp(d)
            zv = z_ref[k, :, ls]
            sv = s_ref[k, :, ls]
            pack_ref[dst, pl.ds(g, 1), :] = top
            pack_ref[dst, pl.ds(groups + g, 1), :] = jnp.sum(a * zv, axis=0, keepdims=True)
            pack_ref[dst, pl.ds(2 * groups + g, 1), :] = jnp.sum(a * (sv + d * zv), axis=0, keepdims=True)
            pack_ref[dst, pl.ds(3 * groups + g, 1), :] = jnp.sum(t_ref[k, :, ls], axis=0, keepdims=True)

    sends = []
    for j in range(1, n_dev):
        peer = lax.rem(me + j, n_dev)
        c = pltpu.make_async_remote_copy(
            src_ref=pack_ref, dst_ref=all_ref.at[j - 1], send_sem=st_send.at[j - 1], recv_sem=st_recv.at[j - 1],
            device_id={"vp": peer}, device_id_type=MESH,
        )
        c.start()
        sends.append(c)
    for c in sends:
        c.wait_recv()
    for c in (to_partner, right_a, left_b, right_b, left_a, fwd_a, fwd_b, *relay, *sends):
        c.wait_send()

    total = jnp.zeros((1, 1), jnp.float32)
    for a in range(n_chip):
        parts = [pack_ref[a]] + [all_ref[j, a] for j in range(n_dev - 1)]
        ms = [p[0:groups] for p in parts]
        top = functools.reduce(jnp.maximum, ms)
        zsum = jnp.zeros_like(top)
        ssum = jnp.zeros_like(top)
        tsum = jnp.zeros_like(top)
        for p, m in zip(parts, ms):
            d = jnp.maximum(m - top, -200.0)
            e = jnp.exp(d)
            zsum = zsum + e * p[groups : 2 * groups]
            ssum = ssum + e * (p[2 * groups : 3 * groups] + d * p[groups : 2 * groups])
            tsum = tsum + p[3 * groups : 4 * groups]
        logz = jnp.log(zsum)
        lp = (tsum - top) - logz
        lp_ref[a] = lp
        ent_ref[a] = logz - ssum / zsum
        total = total + jnp.sum(lp, keepdims=True)
    mean_ref[...] = total / (n_chip * chip_rows)


def solution(mesh):
    n_dev = mesh.shape["vp"]

    def local_step(hidden, target, norm_gain, head_weight):
        own, depth = hidden.shape
        n_chip = n_dev // 2
        chip_rows = 2 * own
        groups = chip_rows // LANES
        vmem = pl.BlockSpec(memory_space=pltpu.VMEM)
        f32 = jnp.float32
        stat = pltpu.VMEM((n_chip, SUBLANES, chip_rows), f32)
        lp, ent, mean = pl.pallas_call(
            functools.partial(kernel, n_dev),
            out_shape=[
                jax.ShapeDtypeStruct((n_chip, groups, LANES), f32),
                jax.ShapeDtypeStruct((n_chip, groups, LANES), f32),
                jax.ShapeDtypeStruct((1, 1), f32),
            ],
            in_specs=[vmem, vmem, vmem, pl.BlockSpec(memory_space=pl.ANY)],
            out_specs=[vmem, vmem, vmem],
            scratch_shapes=[
                pltpu.VMEM((n_chip, chip_rows, depth), jnp.bfloat16),
                pltpu.VMEM((NBUF, PER_TILE * SUB, depth), jnp.bfloat16),
                stat, stat, stat, stat,
                pltpu.VMEM((n_chip, SUBLANES, chip_rows), jnp.int32),
                pltpu.VMEM((SUB, chip_rows), f32),
                pltpu.VMEM((SUB, chip_rows), f32),
                pltpu.VMEM((n_chip, 4 * groups, LANES), f32),
                pltpu.VMEM((n_dev - 1, n_chip, 4 * groups, LANES), f32),
                pltpu.SemaphoreType.DMA((NBUF,)),
                pltpu.SemaphoreType.DMA((13,)),
                pltpu.SemaphoreType.DMA((13,)),
                pltpu.SemaphoreType.DMA((n_dev - 1,)),
                pltpu.SemaphoreType.DMA((n_dev - 1,)),
            ],
            compiler_params=pltpu.CompilerParams(
                collective_id=0, has_side_effects=True, vmem_limit_bytes=67043328
            ),
        )(hidden, target.reshape(n_chip, groups, LANES), norm_gain, head_weight.T)
        return lp.reshape(-1), ent.reshape(-1), mean.reshape(-1)

    return jax.shard_map(
        local_step,
        mesh=mesh,
        in_specs=(P(("dp", "vp"), None), P("dp"), P(None), P(None, "vp")),
        out_specs=(P("dp"), P("dp"), P("dp")),
        check_vma=False,
    )
```

```python
import functools

import jax
import jax.numpy as jnp
from jax import lax
from jax.experimental import pallas as pl
from jax.experimental.pallas import tpu as pltpu
from jax.sharding import PartitionSpec as P

NORM_EPS = 1e-6
LANES = 128
SUBLANES = 8
SUB = 528
HOIST = 32
FOLD = 24
PER_TILE = 2
NBUF = 4
RAW_CHUNKS = 4
LOWEST = float(jnp.finfo(jnp.float32).min)
MESH = pl.DeviceIdType.MESH


def kernel(
    n_dev, hidden_ref, target_ref, gain_ref, head_ref,
    out_ref,
    raw_ref, rows_ref, w_ref, m_ref, z_ref, s_ref, t_ref, id_ref, buf_a, buf_b,
    pack_ref, part_ref, merged_ref, all_ref, fin_ref,
    raw_sem, w_sem, send_sem, recv_sem, st_send, st_recv,
):
    own = hidden_ref.shape[0]
    half = own // 2
    chip_rows = 2 * own
    n_chip = n_dev // 2
    vocab = head_ref.shape[0]
    tile = PER_TILE * SUB
    tiles = vocab // tile
    pairs = tiles // 2
    groups = chip_rows // LANES
    me = lax.axis_index("vp")
    core = lax.rem(me, 2)
    chip = me // 2
    partner = me + 1 - 2 * core
    right = lax.rem(me + 2, n_dev)
    left = lax.rem(me + n_dev - 2, n_dev)

    def w_copy(g):
        row = lax.rem(g, tiles) * tile
        slot = lax.rem(g, NBUF)
        return pltpu.make_async_copy(
            head_ref.at[pl.ds(pl.multiple_of(row, tile), tile), :], w_ref.at[slot], w_sem.at[slot]
        )

    chunk = own // RAW_CHUNKS

    def raw_copy(c):
        rs = pl.ds(c * chunk, chunk)
        return pltpu.make_async_copy(hidden_ref.at[rs, :], raw_ref.at[rs, :], raw_sem.at[c])

    for c in range(RAW_CHUNKS):
        raw_copy(c).start()
    w_copy(0).start()
    w_copy(1).start()

    barrier = pltpu.get_barrier_semaphore()
    for j in range(1, n_dev):
        pl.semaphore_signal(barrier, inc=1, device_id={"vp": lax.rem(me + j, n_dev)}, device_id_type=MESH)

    gain = gain_ref[...].astype(jnp.float32).reshape(1, gain_ref.shape[-1])
    step = 16

    def norm(i, carry):
        x = raw_ref[pl.ds(pl.multiple_of(i * step, step), step), :].astype(jnp.float32)
        inv = lax.rsqrt(jnp.mean(x * x, axis=-1, keepdims=True) + NORM_EPS)
        rows_ref[0, pl.ds(pl.multiple_of(core * own + i * step, step), step), :] = (x * inv * gain).astype(jnp.bfloat16)
        return carry

    for c in range(RAW_CHUNKS):
        raw_copy(c).wait()
        lax.fori_loop(c * chunk // step, (c + 1) * chunk // step, norm, 0)
    pl.semaphore_wait(barrier, n_dev - 1)

    def remote(src, dst, idx, device):
        return pltpu.make_async_remote_copy(
            src_ref=src, dst_ref=dst, send_sem=send_sem.at[idx], recv_sem=recv_sem.at[idx],
            device_id={"vp": device}, device_id_type=MESH,
        )

    mine = pl.multiple_of(core * own, own)

    def piece(slot, part):
        return rows_ref.at[slot, pl.ds(pl.multiple_of(core * own + part * half, half), half), :]

    whole = rows_ref.at[0, pl.ds(mine, own), :]
    to_partner = remote(whole, whole, 0, partner)
    right_a = remote(piece(0, 0), piece(3, 0), 1, right)
    left_b = remote(piece(0, 1), piece(1, 1), 2, left)
    right_b = remote(piece(0, 1), piece(3, 1), 3, right)
    left_a = remote(piece(0, 0), piece(1, 0), 4, left)
    fwd_a = remote(piece(3, 0), piece(2, 0), 5, right)
    fwd_b = remote(piece(1, 1), piece(2, 1), 6, left)
    relay = [
        remote(piece(slot, part), piece(slot, part), 7 + i, partner)
        for i, (slot, part) in enumerate([(3, 0), (1, 1), (3, 1), (1, 0), (2, 0), (2, 1)])
    ]
    to_partner.start()
    right_a.start()
    left_b.start()
    right_b.start()
    left_a.start()

    sublane = lax.broadcasted_iota(jnp.int32, (SUBLANES, LANES), 0)
    for k in range(n_chip):
        src = lax.rem(chip + k, n_chip)
        for g in range(groups):
            ids = target_ref[src, pl.ds(g, 1), :] - me * vocab
            ids = jnp.where((ids >= 0) & (ids < vocab), ids, -(2**29))
            id_ref[k, g] = ids - sublane
    m_ref[...] = jnp.full(m_ref.shape, LOWEST, jnp.float32)
    z_ref[...] = jnp.zeros(z_ref.shape, jnp.float32)
    s_ref[...] = jnp.zeros(s_ref.shape, jnp.float32)
    t_ref[...] = jnp.zeros(t_ref.shape, jnp.float32)

    row_of = lax.broadcasted_iota(jnp.int32, (FOLD, LANES), 0) // SUBLANES * SUBLANES

    def fold(buf, k, base, columns):
        per = SUB // FOLD
        for col, starts in columns:

            def logits(r):
                return buf[pl.ds(r % per * FOLD, FOLD), pl.ds(starts[r // per], LANES)]

            def split(v):
                return [v[i : i + SUBLANES] for i in range(0, FOLD, SUBLANES)]

            def spread(v):
                return jnp.concatenate([v] * (FOLD // SUBLANES), axis=0)

            count = per * len(starts)
            m_old = m_ref[k, col]
            m_new = functools.reduce(jnp.maximum, [*split(functools.reduce(jnp.maximum, map(logits, range(count)))), m_old])
            m_all = spread(m_new)
            ids = spread(id_ref[k, col] - base) - row_of
            zv = sv = jnp.zeros((FOLD, LANES), jnp.float32)
            tv = jnp.zeros((FOLD, LANES), jnp.float32)
            for r in range(count):
                v = logits(r)
                d = v - m_all
                p = jnp.exp(d)
                zv = zv + p
                sv = sv + p * d
                tv = jnp.where(ids == r * FOLD, v, tv)
            d = jnp.maximum(m_old - m_new, -200.0)
            a = jnp.exp(d)
            z_old = z_ref[k, col]
            m_ref[k, col] = m_new
            z_ref[k, col] = functools.reduce(jnp.add, split(zv), a * z_old)
            s_ref[k, col] = functools.reduce(jnp.add, split(sv), a * (s_ref[k, col] + d * z_old))
            t_ref[k, col] = functools.reduce(jnp.add, split(tv), t_ref[k, col])

    def epilogue(buf, k, base):
        fold(buf, k, base, [(g, [g * LANES]) for g in range(groups)])

    def block(k, slot, c, buf):
        buf[...] = lax.dot_general(
            w_ref[slot, pl.ds(c, SUB), :], rows_ref[k], (((1,), (1,)), ((), ())), preferred_element_type=jnp.float32
        )

    bufs = (buf_a, buf_b)

    w_copy(2).start()
    w_copy(3).start()

    def columns(h):
        n = own // LANES
        at = lax.rem(core + h, 2) * n
        return [(at + g, [p * own + g * LANES for p in range(PER_TILE)]) for g in range(n)]

    buf_b[...] = jnp.full(buf_b.shape, LOWEST, jnp.float32)

    def head(h, carry):
        @pl.when(h == 0)
        def _():
            w_copy(0).wait()
            w_copy(1).wait()

        @pl.when(h == 1)
        def _():
            to_partner.wait_recv()

        at = pl.multiple_of(lax.rem(core + h, 2) * own, own)
        for b in range(2):
            v = lax.dot_general(
                w_ref[b], rows_ref[0, pl.ds(at, own), :], (((1,), (1,)), ((), ())), preferred_element_type=jnp.float32
            )
            for p in range(PER_TILE):
                bufs[b][:, pl.ds(p * own, own)] = v[p * SUB : (p + 1) * SUB]
            if b:
                fold(buf_a, 0, 0, columns(h))
            else:
                fold(buf_b, 0, jnp.where(h == 0, -(2**28), tile), columns(h + 1))
        return carry

    lax.fori_loop(0, 2, head, 0)
    fold(buf_b, 0, tile, columns(1))
    buf_b[...] = jnp.full(buf_b.shape, LOWEST, jnp.float32)

    def first(i, carry):
        w_copy(2 * i + 2).start()
        w_copy(2 * i + 3).start()

        @pl.when(i == pairs * 3 // 9)
        def _():
            right_a.wait_recv()
            left_b.wait_recv()
            fwd_a.start()
            fwd_b.start()
            relay[0].start()
            relay[1].start()

        @pl.when(i == pairs * 6 // 9)
        def _():
            right_b.wait_recv()
            left_a.wait_recv()
            relay[2].start()
            relay[3].start()

        @pl.when(i == pairs - 1)
        def _():
            fwd_a.wait_recv()
            fwd_b.wait_recv()
            relay[4].start()
            relay[5].start()

        w_copy(2 * i).wait()
        w_copy(2 * i + 1).wait()
        for b in range(2 * PER_TILE):
            block(0, lax.rem(2 * i + b // PER_TILE, NBUF), (b % PER_TILE) * SUB, bufs[b % 2])
            base = i * 2 * tile + (b - 1) * SUB
            if b == 0:
                base = jnp.where(i == 1, -(2**28), base)
            epilogue(bufs[(b + 1) % 2], 0, base)
        return carry

    lax.fori_loop(1, pairs, first, 0)
    for r in relay:
        r.wait_recv()

    order = [(k, c) for c in range(0, tile, SUB) for k in range(1, n_chip)]

    def second(j, carry):
        g = tiles + j

        @pl.when(j < tiles - 2)
        def _():
            w_copy(g + 2).start()

        w_copy(g).wait()
        for b, (k, c) in enumerate(order):
            block(k, lax.rem(g, NBUF), c, bufs[b % 2])
            pk, pc = order[b - 1]
            base = j * tile + pc
            if b == 0:
                pk = jnp.where(j == 0, 0, pk)
                base = jnp.where(j == 0, vocab - SUB, base - tile)
            epilogue(bufs[(b + 1) % 2], pk, base)
        return carry

    lax.fori_loop(0, tiles, second, 0)
    epilogue(buf_b, n_chip - 1, vocab - SUB)

    for k in range(n_chip):
        dst = lax.rem(chip + k, n_chip)
        for g in range(groups):
            m = m_ref[k, g]
            top = jnp.max(m, axis=0, keepdims=True)
            d = jnp.maximum(m - top, -200.0)
            a = jnp.exp(d)
            zv = z_ref[k, g]
            sv = s_ref[k, g]
            pack_ref[dst, pl.ds(g, 1), :] = top
            pack_ref[dst, pl.ds(groups + g, 1), :] = jnp.sum(a * zv, axis=0, keepdims=True)
            pack_ref[dst, pl.ds(2 * groups + g, 1), :] = jnp.sum(a * (sv + d * zv), axis=0, keepdims=True)
            pack_ref[dst, pl.ds(3 * groups + g, 1), :] = jnp.sum(t_ref[k, g], axis=0, keepdims=True)

    hc = n_chip // 2
    first_chip = core * hc

    def exchange(src, dst, idx, device):
        return pltpu.make_async_remote_copy(
            src_ref=src, dst_ref=dst, send_sem=st_send.at[idx], recv_sem=st_recv.at[idx],
            device_id={"vp": device}, device_id_type=MESH,
        )

    def merge(parts):
        cut = [[p[q * groups : (q + 1) * groups] for q in range(4)] for p in parts]
        top = functools.reduce(jnp.maximum, [c[0] for c in cut])
        zsum = jnp.zeros_like(top)
        ssum = jnp.zeros_like(top)
        tsum = jnp.zeros_like(top)
        for m, zv, sv, tv in cut:
            d = jnp.maximum(m - top, -200.0)
            e = jnp.exp(d)
            zsum = zsum + e * zv
            ssum = ssum + e * (sv + d * zv)
            tsum = tsum + tv
        return top, zsum, ssum, tsum

    swap = exchange(pack_ref.at[pl.ds((1 - core) * hc, hc)], part_ref, 0, partner)
    swap.start()
    swap.wait_recv()
    for a in range(hc):
        for q, v in enumerate(merge([pack_ref[first_chip + a], part_ref[a]])):
            merged_ref[a, q * groups : (q + 1) * groups, :] = v
    across = [exchange(merged_ref, all_ref.at[j - 1], j, lax.rem(me + 2 * j, n_dev)) for j in range(1, n_chip)]
    for c in across:
        c.start()
    for c in across:
        c.wait_recv()
    for a in range(hc):
        top, zsum, ssum, tsum = merge([merged_ref[a]] + [all_ref[j, a] for j in range(n_chip - 1)])
        logz = jnp.log(zsum)
        fin_ref[first_chip + a, 0] = (tsum - top) - logz
        fin_ref[first_chip + a, 1] = logz - ssum / zsum
    done = fin_ref.at[pl.ds(first_chip, hc)]
    give = exchange(done, done, n_chip, partner)
    give.start()
    give.wait_recv()
    for c in (to_partner, right_a, left_b, right_b, left_a, fwd_a, fwd_b, *relay, swap, *across, give):
        c.wait_send()
    out_ref[...] = fin_ref[...]


def finish(res_ref, lp_ref, ent_ref, mean_ref):
    total = jnp.zeros(lp_ref.shape[1:], jnp.float32)
    for a in range(lp_ref.shape[0]):
        lp_ref[a] = res_ref[a, 0]
        ent_ref[a] = res_ref[a, 1]
        total = total + res_ref[a, 0]
    mean_ref[...] = jnp.sum(total, keepdims=True) / lp_ref.size


def solution(mesh):
    n_dev = mesh.shape["vp"]

    def local_step(hidden, target, norm_gain, head_weight):
        own, depth = hidden.shape
        n_chip = n_dev // 2
        chip_rows = 2 * own
        groups = chip_rows // LANES
        vmem = pl.BlockSpec(memory_space=pltpu.VMEM)
        f32 = jnp.float32
        stat = pltpu.VMEM((n_chip, groups, SUBLANES, LANES), f32)
        hbm = pl.BlockSpec(memory_space=pl.ANY)
        res = pl.pallas_call(
            functools.partial(kernel, n_dev),
            out_shape=jax.ShapeDtypeStruct((n_chip, 2, groups, LANES), f32),
            in_specs=[hbm, vmem, vmem, hbm],
            out_specs=vmem,
            scratch_shapes=[
                pltpu.VMEM((own, depth), jnp.bfloat16),
                pltpu.VMEM((n_chip, chip_rows, depth), jnp.bfloat16),
                pltpu.VMEM((NBUF, PER_TILE * SUB, depth), jnp.bfloat16),
                stat, stat, stat, stat,
                pltpu.VMEM((n_chip, groups, SUBLANES, LANES), jnp.int32),
                pltpu.VMEM((SUB, chip_rows), f32),
                pltpu.VMEM((SUB, chip_rows), f32),
                pltpu.VMEM((n_chip, 4 * groups, LANES), f32),
                pltpu.VMEM((n_chip // 2, 4 * groups, LANES), f32),
                pltpu.VMEM((n_chip // 2, 4 * groups, LANES), f32),
                pltpu.VMEM((n_chip - 1, n_chip // 2, 4 * groups, LANES), f32),
                pltpu.VMEM((n_chip, 2, groups, LANES), f32),
                pltpu.SemaphoreType.DMA((RAW_CHUNKS,)),
                pltpu.SemaphoreType.DMA((NBUF,)),
                pltpu.SemaphoreType.DMA((13,)),
                pltpu.SemaphoreType.DMA((13,)),
                pltpu.SemaphoreType.DMA((n_chip + 1,)),
                pltpu.SemaphoreType.DMA((n_chip + 1,)),
            ],
            compiler_params=pltpu.CompilerParams(
                collective_id=0, has_side_effects=True,
                vmem_limit_bytes=67043328
            ),
        )(hidden, target.reshape(n_chip, groups, LANES), norm_gain, head_weight.T)
        lp, ent, mean = pl.pallas_call(
            finish,
            out_shape=[
                jax.ShapeDtypeStruct((n_chip, groups, LANES), f32),
                jax.ShapeDtypeStruct((n_chip, groups, LANES), f32),
                jax.ShapeDtypeStruct((1, 1), f32),
            ],
        )(res)
        return lp.reshape(-1), ent.reshape(-1), mean.reshape(-1)

    return jax.shard_map(
        local_step,
        mesh=mesh,
        in_specs=(P(("dp", "vp"), None), P("dp"), P(None), P(None, "vp")),
        out_specs=(P("dp"), P("dp"), P("dp")),
        check_vma=False,
    )
```

```python
import functools

import jax
import jax.numpy as jnp
from jax import lax
from jax.experimental import pallas as pl
from jax.experimental.pallas import tpu as pltpu
from jax.sharding import PartitionSpec as P

NORM_EPS = 1e-6
LANES = 128
SUBLANES = 8
SUB = 528
HOIST = 32
FOLD = 16
PER_TILE = 2
NBUF = 4
RAW_CHUNKS = 4
LOWEST = float(jnp.finfo(jnp.float32).min)
MESH = pl.DeviceIdType.MESH


def kernel(
    n_dev, hidden_ref, target_ref, gain_ref, head_ref,
    out_ref,
    raw_ref, rows_ref, w_ref, m_ref, z_ref, s_ref, t_ref, id_ref, buf_a, buf_b,
    pack_ref, part_ref, merged_ref, all_ref, fin_ref,
    raw_sem, w_sem, send_sem, recv_sem, st_send, st_recv,
):
    own = hidden_ref.shape[0]
    half = own // 2
    chip_rows = 2 * own
    n_chip = n_dev // 2
    vocab = head_ref.shape[0]
    tile = PER_TILE * SUB
    tiles = vocab // tile
    pairs = tiles // 2
    groups = chip_rows // LANES
    me = lax.axis_index("vp")
    core = lax.rem(me, 2)
    chip = me // 2
    partner = me + 1 - 2 * core
    right = lax.rem(me + 2, n_dev)
    left = lax.rem(me + n_dev - 2, n_dev)

    def w_copy(g):
        row = lax.rem(g, tiles) * tile
        slot = lax.rem(g, NBUF)
        return pltpu.make_async_copy(
            head_ref.at[pl.ds(pl.multiple_of(row, tile), tile), :], w_ref.at[slot], w_sem.at[slot]
        )

    chunk = own // RAW_CHUNKS

    def raw_copy(c):
        rs = pl.ds(c * chunk, chunk)
        return pltpu.make_async_copy(hidden_ref.at[rs, :], raw_ref.at[rs, :], raw_sem.at[c])

    for c in range(RAW_CHUNKS):
        raw_copy(c).start()
    w_copy(0).start()
    w_copy(1).start()

    barrier = pltpu.get_barrier_semaphore()
    for j in range(1, n_dev):
        pl.semaphore_signal(barrier, inc=1, device_id={"vp": lax.rem(me + j, n_dev)}, device_id_type=MESH)

    gain = gain_ref[...].astype(jnp.float32).reshape(1, gain_ref.shape[-1])
    step = 16

    def norm(i, carry):
        x = raw_ref[pl.ds(pl.multiple_of(i * step, step), step), :].astype(jnp.float32)
        inv = lax.rsqrt(jnp.mean(x * x, axis=-1, keepdims=True) + NORM_EPS)
        rows_ref[0, pl.ds(pl.multiple_of(core * own + i * step, step), step), :] = (x * inv * gain).astype(jnp.bfloat16)
        return carry

    for c in range(RAW_CHUNKS):
        raw_copy(c).wait()
        lax.fori_loop(c * chunk // step, (c + 1) * chunk // step, norm, 0)
    pl.semaphore_wait(barrier, n_dev - 1)

    def remote(src, dst, idx, device):
        return pltpu.make_async_remote_copy(
            src_ref=src, dst_ref=dst, send_sem=send_sem.at[idx], recv_sem=recv_sem.at[idx],
            device_id={"vp": device}, device_id_type=MESH,
        )

    mine = pl.multiple_of(core * own, own)

    def piece(slot, part):
        return rows_ref.at[slot, pl.ds(pl.multiple_of(core * own + part * half, half), half), :]

    whole = rows_ref.at[0, pl.ds(mine, own), :]
    to_partner = remote(whole, whole, 0, partner)
    right_a = remote(piece(0, 0), piece(3, 0), 1, right)
    left_b = remote(piece(0, 1), piece(1, 1), 2, left)
    right_b = remote(piece(0, 1), piece(3, 1), 3, right)
    left_a = remote(piece(0, 0), piece(1, 0), 4, left)
    fwd_a = remote(piece(3, 0), piece(2, 0), 5, right)
    fwd_b = remote(piece(1, 1), piece(2, 1), 6, left)
    relay = [
        remote(piece(slot, part), piece(slot, part), 7 + i, partner)
        for i, (slot, part) in enumerate([(3, 0), (1, 1), (3, 1), (1, 0), (2, 0), (2, 1)])
    ]
    to_partner.start()
    right_a.start()
    left_b.start()
    right_b.start()
    left_a.start()

    sublane = lax.broadcasted_iota(jnp.int32, (SUBLANES, LANES), 0)
    for k in range(n_chip):
        src = lax.rem(chip + k, n_chip)
        for g in range(groups):
            ids = target_ref[src, pl.ds(g, 1), :] - me * vocab
            ids = jnp.where((ids >= 0) & (ids < vocab), ids, -(2**29))
            id_ref[k, g] = ids - sublane
    m_ref[...] = jnp.full(m_ref.shape, LOWEST, jnp.float32)
    z_ref[...] = jnp.zeros(z_ref.shape, jnp.float32)
    s_ref[...] = jnp.zeros(s_ref.shape, jnp.float32)
    t_ref[...] = jnp.zeros(t_ref.shape, jnp.float32)

    row_of = lax.broadcasted_iota(jnp.int32, (FOLD, LANES), 0) // SUBLANES * SUBLANES

    def fold(buf, k, base, columns):
        per = SUB // FOLD
        for col, starts in columns:

            def logits(r):
                return buf[pl.ds(r % per * FOLD, FOLD), pl.ds(starts[r // per], LANES)]

            def split(v):
                return [v[i : i + SUBLANES] for i in range(0, FOLD, SUBLANES)]

            def spread(v):
                return jnp.concatenate([v] * (FOLD // SUBLANES), axis=0)

            count = per * len(starts)
            m_old = m_ref[k, col]
            m_new = functools.reduce(jnp.maximum, [*split(functools.reduce(jnp.maximum, map(logits, range(count)))), m_old])
            m_all = spread(m_new)
            ids = spread(id_ref[k, col] - base) - row_of
            zv = sv = jnp.zeros((FOLD, LANES), jnp.float32)
            tv = jnp.zeros((FOLD, LANES), jnp.float32)
            for r in range(count):
                v = logits(r)
                d = v - m_all
                p = jnp.exp(d)
                zv = zv + p
                sv = sv + p * d
                tv = jnp.where(ids == r * FOLD, v, tv)
            d = jnp.maximum(m_old - m_new, -200.0)
            a = jnp.exp(d)
            z_old = z_ref[k, col]
            m_ref[k, col] = m_new
            z_ref[k, col] = functools.reduce(jnp.add, split(zv), a * z_old)
            s_ref[k, col] = functools.reduce(jnp.add, split(sv), a * (s_ref[k, col] + d * z_old))
            t_ref[k, col] = functools.reduce(jnp.add, split(tv), t_ref[k, col])

    def epilogue(buf, k, base):
        fold(buf, k, base, [(g, [g * LANES]) for g in range(groups)])

    def block(k, slot, c, buf):
        buf[...] = lax.dot_general(
            w_ref[slot, pl.ds(c, SUB), :], rows_ref[k], (((1,), (1,)), ((), ())), preferred_element_type=jnp.float32
        )

    bufs = (buf_a, buf_b)

    w_copy(2).start()
    w_copy(3).start()

    def columns(h):
        n = own // LANES
        at = lax.rem(core + h, 2) * n
        return [(at + g, [p * own + g * LANES for p in range(PER_TILE)]) for g in range(n)]

    buf_b[...] = jnp.full(buf_b.shape, LOWEST, jnp.float32)

    def head(h, carry):
        @pl.when(h == 0)
        def _():
            w_copy(0).wait()
            w_copy(1).wait()

        @pl.when(h == 1)
        def _():
            to_partner.wait_recv()

        at = pl.multiple_of(lax.rem(core + h, 2) * own, own)
        for b in range(2):
            v = lax.dot_general(
                w_ref[b], rows_ref[0, pl.ds(at, own), :], (((1,), (1,)), ((), ())), preferred_element_type=jnp.float32
            )
            for p in range(PER_TILE):
                bufs[b][:, pl.ds(p * own, own)] = v[p * SUB : (p + 1) * SUB]
            if b:
                fold(buf_a, 0, 0, columns(h))
            else:
                fold(buf_b, 0, jnp.where(h == 0, -(2**28), tile), columns(h + 1))
        return carry

    lax.fori_loop(0, 2, head, 0)
    fold(buf_b, 0, tile, columns(1))
    buf_b[...] = jnp.full(buf_b.shape, LOWEST, jnp.float32)

    def first(i, carry):
        w_copy(2 * i + 2).start()
        w_copy(2 * i + 3).start()

        @pl.when(i == pairs * 4 // 9)
        def _():
            right_a.wait_recv()
            left_b.wait_recv()
            fwd_a.start()
            fwd_b.start()
            relay[0].start()
            relay[1].start()

        @pl.when(i == pairs * 7 // 9)
        def _():
            right_b.wait_recv()
            left_a.wait_recv()
            relay[2].start()
            relay[3].start()

        @pl.when(i == pairs)
        def _():
            relay[1].wait_recv()
            relay[3].wait_recv()

        @pl.when(i == pairs * 12 // 9)
        def _():
            fwd_a.wait_recv()
            fwd_b.wait_recv()
            relay[4].start()
            relay[5].start()

        w_copy(2 * i).wait()
        w_copy(2 * i + 1).wait()
        second_slot = i >= pairs
        k = jnp.where(second_slot, 1, 0)
        start = (i - jnp.where(second_slot, pairs, 0)) * 2 * tile
        for b in range(2 * PER_TILE):
            block(k, lax.rem(2 * i + b // PER_TILE, NBUF), (b % PER_TILE) * SUB, bufs[b % 2])
            if b:
                epilogue(bufs[(b + 1) % 2], k, start + (b - 1) * SUB)
            else:
                turn = i == pairs
                base = jnp.where(turn, vocab - SUB, start - SUB)
                epilogue(buf_b, jnp.where(turn, 0, k), jnp.where(i == 1, -(2**28), base))
        return carry

    lax.fori_loop(1, 2 * pairs, first, 0)
    for q in (0, 2, 4, 5):
        relay[q].wait_recv()

    order = [(k, b) for b in range(2 * PER_TILE) for k in range(2, n_chip)]

    def second(j, carry):
        g = 2 * tiles + 2 * j

        @pl.when(j < pairs - 1)
        def _():
            w_copy(g + 2).start()
            w_copy(g + 3).start()

        w_copy(g).wait()
        w_copy(g + 1).wait()
        start = j * 2 * tile
        for n, (k, b) in enumerate(order):
            block(k, lax.rem(g + b // PER_TILE, NBUF), (b % PER_TILE) * SUB, bufs[n % 2])
            if n:
                pk, pb = order[n - 1]
                epilogue(bufs[(n + 1) % 2], pk, start + pb * SUB)
            else:
                turn = j == 0
                epilogue(buf_b, jnp.where(turn, 1, n_chip - 1), jnp.where(turn, vocab, start) - SUB)
        return carry

    lax.fori_loop(0, pairs, second, 0)
    epilogue(buf_b, n_chip - 1, vocab - SUB)

    for k in range(n_chip):
        dst = lax.rem(chip + k, n_chip)
        for g in range(groups):
            m = m_ref[k, g]
            top = jnp.max(m, axis=0, keepdims=True)
            d = jnp.maximum(m - top, -200.0)
            a = jnp.exp(d)
            zv = z_ref[k, g]
            sv = s_ref[k, g]
            pack_ref[dst, pl.ds(g, 1), :] = top
            pack_ref[dst, pl.ds(groups + g, 1), :] = jnp.sum(a * zv, axis=0, keepdims=True)
            pack_ref[dst, pl.ds(2 * groups + g, 1), :] = jnp.sum(a * (sv + d * zv), axis=0, keepdims=True)
            pack_ref[dst, pl.ds(3 * groups + g, 1), :] = jnp.sum(t_ref[k, g], axis=0, keepdims=True)

    hc = n_chip // 2
    first_chip = core * hc

    def exchange(src, dst, idx, device):
        return pltpu.make_async_remote_copy(
            src_ref=src, dst_ref=dst, send_sem=st_send.at[idx], recv_sem=st_recv.at[idx],
            device_id={"vp": device}, device_id_type=MESH,
        )

    def merge(parts):
        cut = [[p[q * groups : (q + 1) * groups] for q in range(4)] for p in parts]
        top = functools.reduce(jnp.maximum, [c[0] for c in cut])
        zsum = jnp.zeros_like(top)
        ssum = jnp.zeros_like(top)
        tsum = jnp.zeros_like(top)
        for m, zv, sv, tv in cut:
            d = jnp.maximum(m - top, -200.0)
            e = jnp.exp(d)
            zsum = zsum + e * zv
            ssum = ssum + e * (sv + d * zv)
            tsum = tsum + tv
        return top, zsum, ssum, tsum

    swap = exchange(pack_ref.at[pl.ds((1 - core) * hc, hc)], part_ref, 0, partner)
    swap.start()
    swap.wait_recv()
    for a in range(hc):
        for q, v in enumerate(merge([pack_ref[first_chip + a], part_ref[a]])):
            merged_ref[a, q * groups : (q + 1) * groups, :] = v
    across = [exchange(merged_ref, all_ref.at[j - 1], j, lax.rem(me + 2 * j, n_dev)) for j in range(1, n_chip)]
    for c in across:
        c.start()
    for c in across:
        c.wait_recv()
    for a in range(hc):
        top, zsum, ssum, tsum = merge([merged_ref[a]] + [all_ref[j, a] for j in range(n_chip - 1)])
        logz = jnp.log(zsum)
        fin_ref[first_chip + a, 0] = (tsum - top) - logz
        fin_ref[first_chip + a, 1] = logz - ssum / zsum
    done = fin_ref.at[pl.ds(first_chip, hc)]
    give = exchange(done, done, n_chip, partner)
    give.start()
    give.wait_recv()
    for c in (to_partner, right_a, left_b, right_b, left_a, fwd_a, fwd_b, *relay, swap, *across, give):
        c.wait_send()
    out_ref[...] = fin_ref[...]


def finish(res_ref, lp_ref, ent_ref, mean_ref):
    total = jnp.zeros(lp_ref.shape[1:], jnp.float32)
    for a in range(lp_ref.shape[0]):
        lp_ref[a] = res_ref[a, 0]
        ent_ref[a] = res_ref[a, 1]
        total = total + res_ref[a, 0]
    mean_ref[...] = jnp.sum(total, keepdims=True) / lp_ref.size


def solution(mesh):
    n_dev = mesh.shape["vp"]

    def local_step(hidden, target, norm_gain, head_weight):
        own, depth = hidden.shape
        n_chip = n_dev // 2
        chip_rows = 2 * own
        groups = chip_rows // LANES
        vmem = pl.BlockSpec(memory_space=pltpu.VMEM)
        f32 = jnp.float32
        stat = pltpu.VMEM((n_chip, groups, SUBLANES, LANES), f32)
        hbm = pl.BlockSpec(memory_space=pl.ANY)
        res = pl.pallas_call(
            functools.partial(kernel, n_dev),
            out_shape=jax.ShapeDtypeStruct((n_chip, 2, groups, LANES), f32),
            in_specs=[hbm, vmem, vmem, hbm],
            out_specs=vmem,
            scratch_shapes=[
                pltpu.VMEM((own, depth), jnp.bfloat16),
                pltpu.VMEM((n_chip, chip_rows, depth), jnp.bfloat16),
                pltpu.VMEM((NBUF, PER_TILE * SUB, depth), jnp.bfloat16),
                stat, stat, stat, stat,
                pltpu.VMEM((n_chip, groups, SUBLANES, LANES), jnp.int32),
                pltpu.VMEM((SUB, chip_rows), f32),
                pltpu.VMEM((SUB, chip_rows), f32),
                pltpu.VMEM((n_chip, 4 * groups, LANES), f32),
                pltpu.VMEM((n_chip // 2, 4 * groups, LANES), f32),
                pltpu.VMEM((n_chip // 2, 4 * groups, LANES), f32),
                pltpu.VMEM((n_chip - 1, n_chip // 2, 4 * groups, LANES), f32),
                pltpu.VMEM((n_chip, 2, groups, LANES), f32),
                pltpu.SemaphoreType.DMA((RAW_CHUNKS,)),
                pltpu.SemaphoreType.DMA((NBUF,)),
                pltpu.SemaphoreType.DMA((13,)),
                pltpu.SemaphoreType.DMA((13,)),
                pltpu.SemaphoreType.DMA((n_chip + 1,)),
                pltpu.SemaphoreType.DMA((n_chip + 1,)),
            ],
            compiler_params=pltpu.CompilerParams(
                collective_id=0, has_side_effects=True,
                vmem_limit_bytes=67043328
            ),
        )(hidden, target.reshape(n_chip, groups, LANES), norm_gain, head_weight.T)
        lp, ent, mean = pl.pallas_call(
            finish,
            out_shape=[
                jax.ShapeDtypeStruct((n_chip, groups, LANES), f32),
                jax.ShapeDtypeStruct((n_chip, groups, LANES), f32),
                jax.ShapeDtypeStruct((1, 1), f32),
            ],
        )(res)
        return lp.reshape(-1), ent.reshape(-1), mean.reshape(-1)

    return jax.shard_map(
        local_step,
        mesh=mesh,
        in_specs=(P(("dp", "vp"), None), P("dp"), P(None), P(None, "vp")),
        out_specs=(P("dp"), P("dp"), P("dp")),
        check_vma=False,
    )
```
